256 devices in a mesh: sec: 16 (over x_hi, z), op: 16 (over y, x_lo, core).
Axes of the slice: x: 4 (x_hi: 2, x_lo: 2; x = x_hi * 2 + x_lo), y: 4, z: 8, core: 2. Of those that a mesh axis runs over, the one named last changes fastest.
Arguments:
- wavefunction: bfloat16 [128, 384, 384], P('sec'), may hold values from -6 to 6
- left_ops: bfloat16 [128, 384, 384], P('op'), may hold values from -0.3125 to 0.3125
- right_ops: bfloat16 [128, 384, 384], P('op'), may hold values from -0.3125 to 0.3125
- charge: int32 [128], P('op'), may hold values from -1 to 1
- couple: int32 [128, 128], P('op', 'sec'), may hold values from 0 to 1, as said below
- amplitude: float32 [128, 128], P('op', 'sec'), may hold values from -0.6 to 0.6
Outputs:
- sigma: float32 [128, 384, 384], P('sec', 'op')
The draws below stay inside these ranges and needn't reach their ends.
Inputs may be any that keep to these rules, and one draw needn't show every extreme that they name: `couple`: 1 where operator k acts into target sector t, else 0.
All inputs are finite; a program needn't handle non-finite values.
Results may differ from the reference program's by a relative error of at most 0.0029.
Values may be sent and summed in bfloat16 or wider, within the bound.
A program may use at most 64 MiB of HBM per device.

```python
import jax
import jax.numpy as jnp
from jax import lax

M = 384
NSEC = 128
K = 128


def draw_couple(key, part):
    levels = 10 + 80 * jnp.arange(NSEC, dtype=jnp.int32) // max(NSEC - 1, 1)
    rolled = jax.random.randint(key, (K, NSEC), 0, 100)
    return (rolled < levels[None, :]).astype(jnp.int32)


def with_ends(entries, stream_key, least, high):
    extent = entries.shape
    place = [jax.random.randint(jax.random.fold_in(stream_key, axis), (), 0, extent[axis]) for axis in range(len(extent))]
    entries = entries.at[tuple(place)].set(least)
    longest = extent.index(max(extent))
    place[longest] = (place[longest] + 1) % extent[longest]
    return entries.at[tuple(place)].set(high)


def block_scale(own_key, dims, cuts, least, top_value):
    factor_of = 1.0
    for dim, shards_of in cuts:
        draws = jax.random.uniform(jax.random.fold_in(jax.random.fold_in(own_key, 6), dim), (shards_of,), jnp.float32, least / len(cuts), top_value / len(cuts))
        factor_of = factor_of * jnp.repeat(jnp.exp(draws), dims[dim] // shards_of).reshape((-1,) + (1,) * (len(dims) - 1 - dim))
    return factor_of


def noise(rng, extent, width, bound, shards=(), held_as=jnp.bfloat16):
    array = width * jax.random.normal(rng, extent, jnp.float32)
    if shards:
        array = array * block_scale(rng, extent, shards, -0.22, 0.18)
    return jnp.clip(array, -bound, bound).astype(held_as)


def setup_inputs(seed: int = 0) -> dict:
    keys = jax.random.split(jax.random.key(seed), 7)
    return {
        "wavefunction": noise(keys[0], (NSEC, M, M), 1.0, 6.0, ((0, 16),)),
        "left_ops": noise(keys[1], (K, M, M), M ** -0.5, 0.3125, ((0, 16),)),
        "right_ops": noise(keys[2], (K, M, M), M ** -0.5, 0.3125, ((0, 16),)),
        "charge": with_ends(jax.random.randint(keys[3], (K,), -1, 2), jax.random.fold_in(keys[3], 1), -1, 1).astype(jnp.int32),
        "couple": draw_couple(jax.random.fold_in(keys[6], 71), 0),
        "amplitude": noise(keys[5], (K, NSEC), 0.1, 0.6, ((0, 16), (1, 16)), jnp.float32),
    }


def reference(wavefunction, left_ops, right_ops, charge, couple, amplitude):
    factor = amplitude * couple.astype(jnp.float32)
    blocks = wavefunction.astype(jnp.float32)

    def apply_op(accumulated, operands):
        left_op, right_op, sector_shift, factor_row = operands
        source = jnp.roll(blocks, sector_shift, axis=0)
        middle = jnp.matmul(left_op.astype(jnp.float32), source).astype(jnp.bfloat16)
        contribution = jnp.matmul(middle.astype(jnp.float32), right_op.astype(jnp.float32).T)
        return accumulated + factor_row[:, None, None] * contribution, None

    initial = jnp.zeros(wavefunction.shape, jnp.float32)
    sigma, unused = lax.scan(apply_op, initial, (left_ops, right_ops, charge, factor))
    return sigma
```

```python
import functools

import jax
import jax.numpy as jnp
from jax import lax
from jax.experimental import pallas as pl
from jax.experimental.pallas import tpu as pltpu
from jax.sharding import PartitionSpec as P

MESH = pl.DeviceIdType.MESH
F32 = jnp.float32
BF16 = jnp.bfloat16

PAIRS = (2, 4, 0, 6)


def kernel(
    charge, couple, amplitude, wave, left, right, out,
    w_a, w_b, w_low, w_high, l_buf, r_buf, middle, part, a_recv, x_send, x_recv, y_sum, y_send, y_recv,
    load_sem, l_sem, r_sem, halo_send, halo_recv, a_ssem, a_rsem, x_ssem, x_rsem, y_ssem, y_rsem,
):
    ops, states = right.shape[0], right.shape[1]
    stripe = out.shape[1]
    secs = lax.axis_size("sec")
    sec = lax.axis_index("sec")
    op = lax.axis_index("op")
    core = op % 2
    x = (op // 2) % 2
    y = op // 4
    sec_right, sec_left = (sec + 1) % secs, (sec + secs - 1) % secs
    core_peer = op + 1 - 2 * core
    x_peer = op + 2 - 4 * x
    y_peers = [((y + d) % 4) * 4 + x * 2 + core for d in (1, 2, 3)]

    barrier = pltpu.get_barrier_semaphore()
    for peer in (
        {"op": core_peer}, {"op": x_peer}, {"op": y_peers[0]}, {"op": y_peers[1]}, {"op": y_peers[2]},
        {"sec": sec_right}, {"sec": sec_left},
    ):
        pl.semaphore_signal(barrier, inc=1, device_id=peer, device_id_type=MESH)

    sides = (1 - x, x)
    load_mid = [
        pltpu.make_async_copy(wave.at[pl.ds(1, 4)], w_a, load_sem.at[0]),
        pltpu.make_async_copy(wave.at[pl.ds(3, 4)], w_b, load_sem.at[1]),
    ]
    load_low = pltpu.make_async_copy(wave.at[pl.ds(0, 3)], w_low.at[pl.ds(1, 3)], load_sem.at[2])
    load_high = pltpu.make_async_copy(wave.at[pl.ds(5, 3)], w_high.at[pl.ds(0, 3)], load_sem.at[3])
    load_l = [
        [
            pltpu.make_async_copy(left.at[k, :, sides[half]], l_buf.at[half, k], l_sem.at[half, k])
            for k in range(ops)
        ]
        for half in range(2)
    ]
    load_r = [
        pltpu.make_async_copy(right.at[k], r_buf.at[:, pl.ds(k * states, states)], r_sem.at[k])
        for k in range(ops)
    ]
    load_mid[0].start()
    for copy in load_l[0] + load_r:
        copy.start()
    for copy in (load_mid[1], load_low, load_high, *load_l[1]):
        copy.start()

    pl.semaphore_wait(barrier, 7)
    halo = [
        pltpu.make_async_remote_copy(
            wave.at[7], w_low.at[0], halo_send.at[0], halo_recv.at[0],
            device_id={"sec": sec_right}, device_id_type=MESH,
        ),
        pltpu.make_async_remote_copy(
            wave.at[0], w_high.at[3], halo_send.at[1], halo_recv.at[1],
            device_id={"sec": sec_left}, device_id_type=MESH,
        ),
    ]
    for copy in halo:
        copy.start()

    def compute(step):
        half, p = divmod(step, 4)
        first = PAIRS[p]
        source = (w_a, w_b, w_low, w_high)[p]
        rows = l_buf.shape[2] * l_buf.shape[3]
        for k in range(ops):
            at = 1 - charge[k]
            blocks = jnp.concatenate([source[at], source[at + 1]], axis=1)
            product = jnp.dot(l_buf[half, k].reshape(rows, states), blocks, preferred_element_type=F32)
            product = product.astype(BF16).astype(F32)
            for j in range(2):
                factor = amplitude[k, first + j] * couple[k, first + j].astype(F32)
                middle[j * rows : (j + 1) * rows, k * states : (k + 1) * states] = (
                    product[:, j * states : (j + 1) * states] * factor
                ).astype(BF16)
        if step == 0:
            for copy in load_r:
                copy.wait()
        total = lax.dot_general(
            middle[...], r_buf[...], (((1,), (1,)), ((), ())), preferred_element_type=F32
        )
        part[step] = total.reshape(part.shape[1:])

    def a_copy(step):
        return pltpu.make_async_remote_copy(
            part.at[step, :, :, pl.ds((1 - core) * stripe, stripe), :],
            a_recv.at[step], a_ssem.at[step], a_rsem.at[step],
            device_id={"op": core_peer}, device_id_type=MESH,
        )

    def x_copy(p):
        return pltpu.make_async_remote_copy(
            x_send.at[p], x_recv.at[p], x_ssem.at[p], x_rsem.at[p],
            device_id={"op": x_peer}, device_id_type=MESH,
        )

    def y_copy(p, d):
        return pltpu.make_async_remote_copy(
            y_send.at[p, (y + d) % 4], y_recv.at[p, d - 1], y_ssem.at[p, d - 1], y_rsem.at[p, d - 1],
            device_id={"op": y_peers[d - 1]}, device_id_type=MESH,
        )

    def reduce(step):
        half, p = divmod(step, 4)
        a_copy(step).wait_recv()
        if half == 1:
            x_copy(p).wait_recv()
        for q in range(4):
            both = [
                part[step, j, q, pl.ds(pl.multiple_of(core * stripe, 8), stripe), :] + a_recv[step, j, q]
                for j in range(2)
            ]
            value = jnp.concatenate(both, axis=0)
            if half == 0:
                x_send[p, q] = value.astype(BF16)
            else:
                value = value + x_recv[p, q].astype(F32)
                y_sum[p, q] = value
                y_send[p, q] = value.astype(BF16)
        if half == 0:
            x_copy(p).start()
        else:
            for d in (2, 1, 3):
                y_copy(p, d).start()

    def finish(p):
        for d in (1, 3, 2):
            y_copy(p, d).wait_recv()
        value = y_sum[p, y]
        for d in (1, 2, 3):
            value = value + y_recv[p, d - 1].astype(F32)
        for j in range(2):
            out[PAIRS[p] + j] = value[j * stripe : (j + 1) * stripe]

    load_mid[0].wait()
    for copy in load_l[0]:
        copy.wait()
    for step in range(8):
        if step == 1:
            load_mid[1].wait()
        if step == 2:
            load_low.wait()
            halo[0].wait_recv()
        if step == 3:
            load_high.wait()
            halo[1].wait_recv()
        if step == 4:
            for copy in load_l[1]:
                copy.wait()
        compute(step)
        a_copy(step).start()
        if step >= 1:
            reduce(step - 1)
        if step >= 6:
            finish(step - 6)
    reduce(7)
    finish(2)
    finish(3)
    for copy in halo:
        copy.wait_send()
    for step in range(8):
        a_copy(step).wait_send()
    for p in range(4):
        x_copy(p).wait_send()
        for d in (1, 2, 3):
            y_copy(p, d).wait_send()


def shards(wavefunction, left_ops, right_ops, charge, couple, amplitude):
    ops, states = left_ops.shape[0], left_ops.shape[1]
    sectors = wavefunction.shape[0]
    stripe = states // lax.axis_size("op")
    left = left_ops.reshape(ops, 4, 2, 2 * stripe, states)
    smem = pl.BlockSpec(memory_space=pltpu.SMEM)
    hbm = pl.BlockSpec(memory_space=pl.ANY)
    dma = pltpu.SemaphoreType.DMA
    block = (states, states)
    return pl.pallas_call(
        kernel,
        out_shape=jax.ShapeDtypeStruct((sectors, stripe, states), F32),
        in_specs=[smem, smem, smem, hbm, hbm, hbm],
        out_specs=pl.BlockSpec(memory_space=pltpu.VMEM),
        scratch_shapes=[
            pltpu.VMEM((4, *block), BF16),
            pltpu.VMEM((4, *block), BF16),
            pltpu.VMEM((4, *block), BF16),
            pltpu.VMEM((4, *block), BF16),
            pltpu.VMEM((2, ops, 4, 2 * stripe, states), BF16),
            pltpu.VMEM((states, ops * states), BF16),
            pltpu.VMEM((states, ops * states), BF16),
            pltpu.VMEM((8, 2, 4, 2 * stripe, states), F32),
            pltpu.VMEM((8, 2, 4, stripe, states), F32),
            pltpu.VMEM((4, 4, 2 * stripe, states), BF16),
            pltpu.VMEM((4, 4, 2 * stripe, states), BF16),
            pltpu.VMEM((4, 4, 2 * stripe, states), F32),
            pltpu.VMEM((4, 4, 2 * stripe, states), BF16),
            pltpu.VMEM((4, 3, 2 * stripe, states), BF16),
            dma((4,)), dma((2, ops)), dma((ops,)), dma((2,)), dma((2,)), dma((8,)), dma((8,)),
            dma((4,)), dma((4,)), dma((4, 3)), dma((4, 3)),
        ],
        compiler_params=pltpu.CompilerParams(
            collective_id=0, has_side_effects=True, vmem_limit_bytes=60000 * 1024
        ),
        name="sigma",
    )(charge, couple, amplitude, wavefunction, left, right_ops)


def solution(mesh):
    placed = (
        P("sec", None, None),
        P("op", None, None),
        P("op", None, None),
        P("op"),
        P("op", "sec"),
        P("op", "sec"),
    )
    return jax.shard_map(
        shards, mesh=mesh, in_specs=placed, out_specs=P("sec", "op", None), check_vma=False
    )
```

```python
import functools

import jax
import jax.numpy as jnp
from jax import lax
from jax.experimental import pallas as pl
from jax.experimental.pallas import tpu as pltpu
from jax.sharding import PartitionSpec as P

MESH = pl.DeviceIdType.MESH
F32 = jnp.float32
BF16 = jnp.bfloat16

PAIRS = (2, 4, 0, 6)
STEPS = ((0, 0), (0, 1), (1, 0), (0, 2), (0, 3), (1, 1), (1, 2), (1, 3))


def kernel(
    charge, couple, amplitude, wave, left, right, out,
    w_a, w_b, w_low, w_high, l_buf, r_buf, middle, part, a_recv, x_send, x_recv, y_sum, y_send, y_recv,
    load_sem, l_sem, r_sem, halo_send, halo_recv, pass_send, pass_recv, a_ssem, a_rsem, x_ssem, x_rsem, y_ssem, y_rsem,
):
    ops, states = right.shape[0], right.shape[1]
    stripe = out.shape[1]
    secs = lax.axis_size("sec")
    sec = lax.axis_index("sec")
    op = lax.axis_index("op")
    core = op % 2
    x = (op // 2) % 2
    y = op // 4
    core_peer = op + 1 - 2 * core
    x_peer = op + 2 - 4 * x
    depth = secs // 2
    to_right = {"sec": (sec + 1) % secs, "op": op + ((sec % depth) // (depth - 1)) * (x_peer - op)}
    to_left = {"sec": (sec + secs - 1) % secs, "op": op + ((depth - 1 - sec % depth) // (depth - 1)) * (x_peer - op)}
    y_peers = [((y + d) % 4) * 4 + x * 2 + core for d in (1, 2, 3)]

    barrier = pltpu.get_barrier_semaphore()
    for peer in (
        {"op": core_peer}, {"op": x_peer}, {"op": y_peers[0]}, {"op": y_peers[1]}, {"op": y_peers[2]},
        to_right, to_left,
    ):
        pl.semaphore_signal(barrier, inc=1, device_id=peer, device_id_type=MESH)

    sides = (1 - x, x)
    load_mid = [
        pltpu.make_async_copy(wave.at[pl.ds(1, 4)], w_a, load_sem.at[0]),
        pltpu.make_async_copy(wave.at[pl.ds(3, 4)], w_b, load_sem.at[1]),
    ]
    load_low = pltpu.make_async_copy(wave.at[pl.ds(0, 3)], w_low.at[pl.ds(1, 3)], load_sem.at[2])
    load_high = pltpu.make_async_copy(wave.at[pl.ds(5, 3)], w_high.at[pl.ds(0, 3)], load_sem.at[3])
    load_l = [
        [
            pltpu.make_async_copy(left.at[k, :, sides[half]], l_buf.at[half, k], l_sem.at[half, k])
            for k in range(ops)
        ]
        for half in range(2)
    ]
    load_r = [
        pltpu.make_async_copy(right.at[k], r_buf.at[:, pl.ds(k * states, states)], r_sem.at[k])
        for k in range(ops)
    ]
    load_mid[0].start()
    for copy in load_l[0] + load_r:
        copy.start()
    for copy in (load_mid[1], load_low, load_high, *load_l[1]):
        copy.start()

    pl.semaphore_wait(barrier, 7)
    half_rows = pl.ds(pl.multiple_of(core * (states // 2), 8), states // 2)
    ends = (w_low.at[0, half_rows], w_high.at[3, half_rows])
    halo = [
        pltpu.make_async_remote_copy(
            wave.at[(7, 0)[side], half_rows], ends[side], halo_send.at[side], halo_recv.at[side],
            device_id=(to_right, to_left)[side], device_id_type=MESH,
        )
        for side in range(2)
    ]
    passed = [
        pltpu.make_async_remote_copy(
            ends[side], ends[side], pass_send.at[side], pass_recv.at[side],
            device_id={"op": core_peer}, device_id_type=MESH,
        )
        for side in range(2)
    ]
    for copy in halo:
        copy.start()

    def compute(step):
        half, p = STEPS[step]
        first = PAIRS[p]
        source = (w_a, w_b, w_low, w_high)[p]
        rows = l_buf.shape[2] * l_buf.shape[3]
        for k in range(ops):
            at = 1 - charge[k]
            blocks = jnp.concatenate([source[at], source[at + 1]], axis=1)
            product = jnp.dot(l_buf[half, k].reshape(rows, states), blocks, preferred_element_type=F32)
            product = product.astype(BF16).astype(F32)
            for j in range(2):
                factor = amplitude[k, first + j] * couple[k, first + j].astype(F32)
                middle[j * rows : (j + 1) * rows, k * states : (k + 1) * states] = (
                    product[:, j * states : (j + 1) * states] * factor
                ).astype(BF16)
        if step == 0:
            for copy in load_r:
                copy.wait()
        total = lax.dot_general(
            middle[...], r_buf[...], (((1,), (1,)), ((), ())), preferred_element_type=F32
        )
        part[step] = total.reshape(part.shape[1:])

    def a_copy(step):
        return pltpu.make_async_remote_copy(
            part.at[step, :, :, pl.ds((1 - core) * stripe, stripe), :],
            a_recv.at[step], a_ssem.at[step], a_rsem.at[step],
            device_id={"op": core_peer}, device_id_type=MESH,
        )

    def x_copy(p):
        return pltpu.make_async_remote_copy(
            x_send.at[p], x_recv.at[p], x_ssem.at[p], x_rsem.at[p],
            device_id={"op": x_peer}, device_id_type=MESH,
        )

    def y_copy(p, d):
        return pltpu.make_async_remote_copy(
            y_send.at[p, (y + d) % 4], y_recv.at[p, d - 1], y_ssem.at[p, d - 1], y_rsem.at[p, d - 1],
            device_id={"op": y_peers[d - 1]}, device_id_type=MESH,
        )

    def reduce(step):
        half, p = STEPS[step]
        a_copy(step).wait_recv()
        if half == 1:
            x_copy(p).wait_recv()
        for q in range(4):
            both = [
                part[step, j, q, pl.ds(pl.multiple_of(core * stripe, 8), stripe), :] + a_recv[step, j, q]
                for j in range(2)
            ]
            value = jnp.concatenate(both, axis=0)
            if half == 0:
                x_send[p, q] = value.astype(BF16)
            else:
                value = value + x_recv[p, q].astype(F32)
                y_sum[p, q] = value
                y_send[p, q] = value.astype(BF16)
        if half == 0:
            x_copy(p).start()
        else:
            for d in (2, 1, 3):
                y_copy(p, d).start()

    def finish(p):
        for d in (1, 3, 2):
            y_copy(p, d).wait_recv()
        value = y_sum[p, y]
        for d in (1, 2, 3):
            value = value + y_recv[p, d - 1].astype(F32)
        for j in range(2):
            out[PAIRS[p] + j] = value[j * stripe : (j + 1) * stripe]

    load_mid[0].wait()
    for copy in load_l[0]:
        copy.wait()
    for step in range(8):
        if step == 1:
            load_mid[1].wait()
        if step == 2:
            for copy in load_l[1]:
                copy.wait()
            for side in range(2):
                halo[side].wait_recv()
                passed[side].start()
        if step == 3:
            load_low.wait()
            load_high.wait()
            for side in range(2):
                passed[side].wait_recv()
        compute(step)
        a_copy(step).start()
        if step >= 1:
            reduce(step - 1)
        if step == 4:
            finish(0)
        if step == 7:
            finish(1)
    reduce(7)
    finish(2)
    finish(3)
    for copy in halo + passed:
        copy.wait_send()
    for step in range(8):
        a_copy(step).wait_send()
    for p in range(4):
        x_copy(p).wait_send()
        for d in (1, 2, 3):
            y_copy(p, d).wait_send()


def shards(wavefunction, left_ops, right_ops, charge, couple, amplitude):
    ops, states = left_ops.shape[0], left_ops.shape[1]
    sectors = wavefunction.shape[0]
    stripe = states // lax.axis_size("op")
    left = left_ops.reshape(ops, 4, 2, 2 * stripe, states)
    smem = pl.BlockSpec(memory_space=pltpu.SMEM)
    hbm = pl.BlockSpec(memory_space=pl.ANY)
    dma = pltpu.SemaphoreType.DMA
    block = (states, states)
    return pl.pallas_call(
        kernel,
        out_shape=jax.ShapeDtypeStruct((sectors, stripe, states), F32),
        in_specs=[smem, smem, smem, hbm, hbm, hbm],
        out_specs=pl.BlockSpec(memory_space=pltpu.VMEM),
        scratch_shapes=[
            pltpu.VMEM((4, *block), BF16),
            pltpu.VMEM((4, *block), BF16),
            pltpu.VMEM((4, *block), BF16),
            pltpu.VMEM((4, *block), BF16),
            pltpu.VMEM((2, ops, 4, 2 * stripe, states), BF16),
            pltpu.VMEM((states, ops * states), BF16),
            pltpu.VMEM((states, ops * states), BF16),
            pltpu.VMEM((8, 2, 4, 2 * stripe, states), F32),
            pltpu.VMEM((8, 2, 4, stripe, states), F32),
            pltpu.VMEM((4, 4, 2 * stripe, states), BF16),
            pltpu.VMEM((4, 4, 2 * stripe, states), BF16),
            pltpu.VMEM((4, 4, 2 * stripe, states), F32),
            pltpu.VMEM((4, 4, 2 * stripe, states), BF16),
            pltpu.VMEM((4, 3, 2 * stripe, states), BF16),
            dma((4,)), dma((2, ops)), dma((ops,)), dma((2,)), dma((2,)), dma((2,)), dma((2,)), dma((8,)), dma((8,)),
            dma((4,)), dma((4,)), dma((4, 3)), dma((4, 3)),
        ],
        compiler_params=pltpu.CompilerParams(
            collective_id=0, has_side_effects=True, vmem_limit_bytes=60000 * 1024
        ),
        name="sigma",
    )(charge, couple, amplitude, wavefunction, left, right_ops)


def solution(mesh):
    placed = (
        P("sec", None, None),
        P("op", None, None),
        P("op", None, None),
        P("op"),
        P("op", "sec"),
        P("op", "sec"),
    )
    return jax.shard_map(
        shards, mesh=mesh, in_specs=placed, out_specs=P("sec", "op", None), check_vma=False
    )
```

```python
import functools

import jax
import jax.numpy as jnp
from jax import lax
from jax.experimental import pallas as pl
from jax.experimental.pallas import tpu as pltpu
from jax.sharding import PartitionSpec as P

MESH = pl.DeviceIdType.MESH
F32 = jnp.float32
BF16 = jnp.bfloat16

PAIRS = ((1, 2), (3, 4), (5, 6), (0, 7))
STEPS = ((0, 0), (0, 1), (0, 2), (1, 0), (1, 1), (0, 3), (1, 2), (1, 3))


def kernel(
    charge, couple, amplitude, wave, left, right, out,
    w_a, w_b, w_c, w_low, w_high, l_buf, r_buf, middle, part, a_recv, x_send, x_recv, y_sum, y_send, y_recv,
    load_sem, l_sem, r_sem, halo_send, halo_recv, pass_send, pass_recv, a_ssem, a_rsem, x_ssem, x_rsem, y_ssem, y_rsem,
):
    ops, states = right.shape[0], right.shape[1]
    stripe = out.shape[1]
    secs = lax.axis_size("sec")
    sec = lax.axis_index("sec")
    op = lax.axis_index("op")
    core = op % 2
    x = (op // 2) % 2
    y = op // 4
    core_peer = op + 1 - 2 * core
    x_peer = op + 2 - 4 * x
    depth = secs // 2
    to_right = {"sec": (sec + 1) % secs, "op": op + ((sec % depth) // (depth - 1)) * (x_peer - op)}
    to_left = {"sec": (sec + secs - 1) % secs, "op": op + ((depth - 1 - sec % depth) // (depth - 1)) * (x_peer - op)}
    y_peers = [((y + d) % 4) * 4 + x * 2 + core for d in (1, 2, 3)]

    barrier = pltpu.get_barrier_semaphore()
    for peer in (
        {"op": core_peer}, {"op": x_peer}, {"op": y_peers[0]}, {"op": y_peers[1]}, {"op": y_peers[2]},
        to_right, to_left,
    ):
        pl.semaphore_signal(barrier, inc=1, device_id=peer, device_id_type=MESH)

    sides = (1 - x, x)
    load_mid = [
        pltpu.make_async_copy(wave.at[pl.ds(2 * p, 4)], (w_a, w_b, w_c)[p], load_sem.at[p]) for p in range(3)
    ]
    load_low = pltpu.make_async_copy(wave.at[pl.ds(0, 2)], w_low.at[pl.ds(1, 2)], load_sem.at[3])
    load_high = pltpu.make_async_copy(wave.at[pl.ds(6, 2)], w_high.at[pl.ds(0, 2)], load_sem.at[4])
    load_l = [
        [
            pltpu.make_async_copy(left.at[k, :, sides[half]], l_buf.at[half, k], l_sem.at[half, k])
            for k in range(ops)
        ]
        for half in range(2)
    ]
    load_r = [
        pltpu.make_async_copy(right.at[k], r_buf.at[:, pl.ds(k * states, states)], r_sem.at[k])
        for k in range(ops)
    ]
    load_mid[0].start()
    for copy in load_l[0] + load_r:
        copy.start()
    for copy in (load_mid[1], load_mid[2], *load_l[1], load_low, load_high):
        copy.start()

    half_rows = pl.ds(pl.multiple_of(core * (states // 2), 8), states // 2)
    ends = (w_low.at[0, half_rows], w_high.at[2, half_rows])
    halo = [
        pltpu.make_async_remote_copy(
            wave.at[(7, 0)[side], half_rows], ends[side], halo_send.at[side], halo_recv.at[side],
            device_id=(to_right, to_left)[side], device_id_type=MESH,
        )
        for side in range(2)
    ]
    passed = [
        pltpu.make_async_remote_copy(
            ends[side], ends[side], pass_send.at[side], pass_recv.at[side],
            device_id={"op": core_peer}, device_id_type=MESH,
        )
        for side in range(2)
    ]

    def enter():
        pl.semaphore_wait(barrier, 7)
        for copy in halo:
            copy.start()

    late = (sec % depth) // (depth // 2)

    def compute(step):
        half, p = STEPS[step]
        low, high, gap = ((w_a, w_a, 1), (w_b, w_b, 1), (w_c, w_c, 1), (w_low, w_high, 0))[p]
        rows = l_buf.shape[2] * l_buf.shape[3]
        for k in range(ops):
            at = 1 - charge[k]
            blocks = jnp.concatenate([low[at], high[at + gap]], axis=1)
            product = jnp.dot(l_buf[half, k].reshape(rows, states), blocks, preferred_element_type=F32)
            product = product.astype(BF16).astype(F32)
            for j in range(2):
                target = PAIRS[p][j]
                factor = amplitude[k, target] * couple[k, target].astype(F32)
                middle[j * rows : (j + 1) * rows, k * states : (k + 1) * states] = (
                    product[:, j * states : (j + 1) * states] * factor
                ).astype(BF16)
        if step == 0:
            for copy in load_r:
                copy.wait()
        total = lax.dot_general(
            middle[...], r_buf[...], (((1,), (1,)), ((), ())), preferred_element_type=F32
        )
        part[step] = total.reshape(part.shape[1:])

    def a_copy(step):
        return pltpu.make_async_remote_copy(
            part.at[step, :, :, pl.ds((1 - core) * stripe, stripe), :],
            a_recv.at[step], a_ssem.at[step], a_rsem.at[step],
            device_id={"op": core_peer}, device_id_type=MESH,
        )

    def x_copy(p):
        return pltpu.make_async_remote_copy(
            x_send.at[p], x_recv.at[p], x_ssem.at[p], x_rsem.at[p],
            device_id={"op": x_peer}, device_id_type=MESH,
        )

    def y_copy(p, d):
        return pltpu.make_async_remote_copy(
            y_send.at[p, (y + d) % 4], y_recv.at[p, d - 1], y_ssem.at[p, d - 1], y_rsem.at[p, d - 1],
            device_id={"op": y_peers[d - 1]}, device_id_type=MESH,
        )

    def reduce(step):
        half, p = STEPS[step]
        a_copy(step).wait_recv()
        if half == 1:
            x_copy(p).wait_recv()
        for q in range(4):
            both = [
                part[step, j, q, pl.ds(pl.multiple_of(core * stripe, 8), stripe), :] + a_recv[step, j, q]
                for j in range(2)
            ]
            value = jnp.concatenate(both, axis=0)
            if half == 0:
                x_send[p, q] = value.astype(BF16)
            else:
                value = value + x_recv[p, q].astype(F32)
                y_sum[p, q] = value
                y_send[p, q] = value.astype(BF16)
        if half == 0:
            x_copy(p).start()
        else:
            for d in (2, 1, 3):
                y_copy(p, d).start()

    def finish(p):
        for d in (1, 3, 2):
            y_copy(p, d).wait_recv()
        value = y_sum[p, y]
        for d in (1, 2, 3):
            value = value + y_recv[p, d - 1].astype(F32)
        for j in range(2):
            out[PAIRS[p][j]] = value[j * stripe : (j + 1) * stripe]

    pl.when(late == 1)(enter)
    load_mid[0].wait()
    for copy in load_l[0]:
        copy.wait()
    for step in range(8):
        if step in (1, 2):
            load_mid[step].wait()
        if step == 3:
            for copy in load_l[1]:
                copy.wait()
        if step == 4:
            for side in range(2):
                halo[side].wait_recv()
                passed[side].start()
        if step == 5:
            load_low.wait()
            load_high.wait()
            for side in range(2):
                passed[side].wait_recv()
        compute(step)
        if step == 0:
            pl.when(late == 0)(enter)
        a_copy(step).start()
        if step >= 1:
            reduce(step - 1)
        if step == 6:
            finish(0)
    reduce(7)
    for p in (1, 2, 3):
        finish(p)
    for copy in halo + passed:
        copy.wait_send()
    for step in range(8):
        a_copy(step).wait_send()
    for p in range(4):
        x_copy(p).wait_send()
        for d in (1, 2, 3):
            y_copy(p, d).wait_send()


def shards(wavefunction, left_ops, right_ops, charge, couple, amplitude):
    ops, states = left_ops.shape[0], left_ops.shape[1]
    sectors = wavefunction.shape[0]
    stripe = states // lax.axis_size("op")
    left = left_ops.reshape(ops, 4, 2, 2 * stripe, states)
    smem = pl.BlockSpec(memory_space=pltpu.SMEM)
    hbm = pl.BlockSpec(memory_space=pl.ANY)
    dma = pltpu.SemaphoreType.DMA
    block = (states, states)
    return pl.pallas_call(
        kernel,
        out_shape=jax.ShapeDtypeStruct((sectors, stripe, states), F32),
        in_specs=[smem, smem, smem, hbm, hbm, hbm],
        out_specs=pl.BlockSpec(memory_space=pltpu.VMEM),
        scratch_shapes=[
            pltpu.VMEM((4, *block), BF16),
            pltpu.VMEM((4, *block), BF16),
            pltpu.VMEM((4, *block), BF16),
            pltpu.VMEM((3, *block), BF16),
            pltpu.VMEM((3, *block), BF16),
            pltpu.VMEM((2, ops, 4, 2 * stripe, states), BF16),
            pltpu.VMEM((states, ops * states), BF16),
            pltpu.VMEM((states, ops * states), BF16),
            pltpu.VMEM((8, 2, 4, 2 * stripe, states), F32),
            pltpu.VMEM((8, 2, 4, stripe, states), F32),
            pltpu.VMEM((4, 4, 2 * stripe, states), BF16),
            pltpu.VMEM((4, 4, 2 * stripe, states), BF16),
            pltpu.VMEM((4, 4, 2 * stripe, states), F32),
            pltpu.VMEM((4, 4, 2 * stripe, states), BF16),
            pltpu.VMEM((4, 3, 2 * stripe, states), BF16),
            dma((5,)), dma((2, ops)), dma((ops,)), dma((2,)), dma((2,)), dma((2,)), dma((2,)), dma((8,)), dma((8,)),
            dma((4,)), dma((4,)), dma((4, 3)), dma((4, 3)),
        ],
        compiler_params=pltpu.CompilerParams(
            collective_id=0, has_side_effects=True, vmem_limit_bytes=60000 * 1024
        ),
        name="sigma",
    )(charge, couple, amplitude, wavefunction, left, right_ops)


def solution(mesh):
    placed = (
        P("sec", None, None),
        P("op", None, None),
        P("op", None, None),
        P("op"),
        P("op", "sec"),
        P("op", "sec"),
    )
    return jax.shard_map(
        shards, mesh=mesh, in_specs=placed, out_specs=P("sec", "op", None), check_vma=False
    )
```

```python
import functools

import jax
import jax.numpy as jnp
from jax import lax
from jax.experimental import pallas as pl
from jax.experimental.pallas import tpu as pltpu
from jax.sharding import PartitionSpec as P

MESH = pl.DeviceIdType.MESH
F32 = jnp.float32
BF16 = jnp.bfloat16

PAIRS = ((1, 2), (3, 4), (5, 6), (0, 7))
STEPS = ((0, 0), (0, 1), (0, 2), (1, 0), (1, 1), (0, 3), (1, 2), (1, 3))
ORDER = (2, 1, 3)


def kernel(
    charge, couple, amplitude, wave, left, right, out,
    w_a, w_b, w_c, w_low, w_high, l_buf, r_buf, middle, own_middle, part, own_part, a_recv, own_recv,
    x_send, x_recv, y_send, y_recv,
    load_sem, l_sem, r_sem, halo_send, halo_recv, pass_send, pass_recv, a_ssem, a_rsem, last_ssem, last_rsem,
    own_sem, x_ssem, x_rsem, y_ssem, y_rsem,
):
    ops, states = right.shape[0], right.shape[1]
    stripe = out.shape[1]
    secs = lax.axis_size("sec")
    sec = lax.axis_index("sec")
    op = lax.axis_index("op")
    core = op % 2
    x = (op // 2) % 2
    y = op // 4
    core_peer = op + 1 - 2 * core
    x_peer = op + 2 - 4 * x
    depth = secs // 2
    to_right = {"sec": (sec + 1) % secs, "op": op + ((sec % depth) // (depth - 1)) * (x_peer - op)}
    to_left = {"sec": (sec + secs - 1) % secs, "op": op + ((depth - 1 - sec % depth) // (depth - 1)) * (x_peer - op)}
    y_peers = [((y + d) % 4) * 4 + x * 2 + core for d in (1, 2, 3)]

    barrier = pltpu.get_barrier_semaphore()
    for peer in (
        {"op": core_peer}, {"op": x_peer}, {"op": y_peers[0]}, {"op": y_peers[1]}, {"op": y_peers[2]},
        to_right, to_left,
    ):
        pl.semaphore_signal(barrier, inc=1, device_id=peer, device_id_type=MESH)

    sides = (1 - x, x)
    load_mid = [
        pltpu.make_async_copy(wave.at[pl.ds(2 * p, 4)], (w_a, w_b, w_c)[p], load_sem.at[p]) for p in range(3)
    ]
    load_low = pltpu.make_async_copy(wave.at[pl.ds(0, 2)], w_low.at[pl.ds(1, 2)], load_sem.at[3])
    load_high = pltpu.make_async_copy(wave.at[pl.ds(6, 2)], w_high.at[pl.ds(0, 2)], load_sem.at[4])
    load_l = [
        [
            pltpu.make_async_copy(left.at[:, (y + d) % 4, sides[half]], l_buf.at[half, d], l_sem.at[half, d])
            for d in range(4)
        ]
        for half in range(2)
    ]
    load_r = [
        pltpu.make_async_copy(right.at[k], r_buf.at[:, pl.ds(k * states, states)], r_sem.at[k])
        for k in range(ops)
    ]
    load_mid[0].start()
    for copy in load_l[0] + load_r:
        copy.start()
    for copy in (load_mid[1], load_mid[2], *load_l[1], load_low, load_high):
        copy.start()

    half_rows = pl.ds(pl.multiple_of(core * (states // 2), 8), states // 2)
    ends = (w_low.at[0, half_rows], w_high.at[2, half_rows])
    halo = [
        pltpu.make_async_remote_copy(
            wave.at[(7, 0)[side], half_rows], ends[side], halo_send.at[side], halo_recv.at[side],
            device_id=(to_right, to_left)[side], device_id_type=MESH,
        )
        for side in range(2)
    ]
    passed = [
        pltpu.make_async_remote_copy(
            ends[side], ends[side], pass_send.at[side], pass_recv.at[side],
            device_id={"op": core_peer}, device_id_type=MESH,
        )
        for side in range(2)
    ]

    def enter():
        pl.semaphore_wait(barrier, 7)
        for copy in halo:
            copy.start()

    late = (sec % depth) // (depth // 2)
    rows = 8 * stripe
    near = 2 * stripe

    def compute(step):
        half, p = STEPS[step]
        low, high, gap = ((w_a, w_a, 1), (w_b, w_b, 1), (w_c, w_c, 1), (w_low, w_high, 0))[p]
        skip = near * half
        kept = rows - skip
        for k in range(ops):
            at = 1 - charge[k]
            columns = slice(k * states, (k + 1) * states)
            blocks = jnp.concatenate([low[at], high[at + gap]], axis=1)
            product = jnp.dot(l_buf[half, :, k].reshape(rows, states), blocks, preferred_element_type=F32)
            product = product.astype(BF16).astype(F32)
            for j in range(2):
                target = PAIRS[p][j]
                factor = amplitude[k, target] * couple[k, target].astype(F32)
                scaled = (product[:, j * states : (j + 1) * states] * factor).astype(BF16)
                middle[j * kept : (j + 1) * kept, columns] = scaled[skip:]
                if half == 1:
                    own_middle[(2 * p + j) * near : (2 * p + j + 1) * near, columns] = scaled[:near]
        if step == 0:
            for copy in load_r:
                copy.wait()
        total = lax.dot_general(
            middle[: 2 * kept], r_buf[...], (((1,), (1,)), ((), ())), preferred_element_type=F32
        )
        part[step, :, half:] = total.reshape(2, 4 - half, near, states)

    def compute_own():
        total = lax.dot_general(
            own_middle[...], r_buf[...], (((1,), (1,)), ((), ())), preferred_element_type=F32
        )
        own_part[...] = total.reshape(own_part.shape)

    other = pl.ds(pl.multiple_of((1 - core) * stripe, 8), stripe)
    mine = pl.ds(pl.multiple_of(core * stripe, 8), stripe)

    def a_copies(step):
        if step == 7:
            return [
                pltpu.make_async_remote_copy(
                    part.at[step, :, d, other, :], a_recv.at[step, :, d], last_ssem.at[d - 1], last_rsem.at[d - 1],
                    device_id={"op": core_peer}, device_id_type=MESH,
                )
                for d in ORDER
            ]
        half = STEPS[step][0]
        return [
            pltpu.make_async_remote_copy(
                part.at[step, :, pl.ds(half, 4 - half), other, :], a_recv.at[step, :, pl.ds(half, 4 - half)],
                a_ssem.at[step], a_rsem.at[step],
                device_id={"op": core_peer}, device_id_type=MESH,
            )
        ]

    def own_copy():
        return pltpu.make_async_remote_copy(
            own_part.at[:, other, :], own_recv, own_sem.at[0], own_sem.at[1],
            device_id={"op": core_peer}, device_id_type=MESH,
        )

    def x_copies(p):
        if p == 3:
            return [
                pltpu.make_async_remote_copy(
                    x_send.at[p, d], x_recv.at[p, d], x_ssem.at[3 + d], x_rsem.at[3 + d],
                    device_id={"op": x_peer}, device_id_type=MESH,
                )
                for d in (*ORDER, 0)
            ]
        return [
            pltpu.make_async_remote_copy(
                x_send.at[p], x_recv.at[p], x_ssem.at[p], x_rsem.at[p],
                device_id={"op": x_peer}, device_id_type=MESH,
            )
        ]

    def y_copy(p, d):
        return pltpu.make_async_remote_copy(
            y_send.at[p, d - 1], y_recv.at[p, d - 1], y_ssem.at[p, d - 1], y_rsem.at[p, d - 1],
            device_id={"op": y_peers[d - 1]}, device_id_type=MESH,
        )

    def reduce(step):
        half, p = STEPS[step]
        core_copies = a_copies(step)
        across = x_copies(p)
        if step != 7:
            core_copies[0].wait_recv()
        if half == 1 and p != 3:
            across[0].wait_recv()
        for i, d in enumerate((*ORDER, 0) if half == 0 else ORDER):
            if step == 7:
                core_copies[i].wait_recv()
            value = jnp.concatenate([part[step, j, d, mine, :] + a_recv[step, j, d] for j in range(2)], axis=0)
            if half == 0:
                x_send[p, d] = value.astype(BF16)
                if p == 3:
                    across[i].start()
            else:
                if p == 3:
                    across[i].wait_recv()
                y_send[p, d - 1] = (value + x_recv[p, d].astype(F32)).astype(BF16)
                y_copy(p, d).start()
        if half == 0 and p != 3:
            across[0].start()

    def finish_own():
        own_copy().wait_recv()
        x_copies(3)[3].wait_recv()
        for p in range(4):
            for j in range(2):
                out[PAIRS[p][j]] = (
                    own_part[2 * p + j, mine, :]
                    + own_recv[2 * p + j]
                    + x_recv[p, 0, j * stripe : (j + 1) * stripe].astype(F32)
                )

    def finish(p):
        for d in (1, 3, 2):
            y_copy(p, d).wait_recv()
        value = y_recv[p, 0].astype(F32) + y_recv[p, 1].astype(F32) + y_recv[p, 2].astype(F32)
        for j in range(2):
            out[PAIRS[p][j]] += value[j * stripe : (j + 1) * stripe]

    pl.when(late == 1)(enter)
    load_mid[0].wait()
    for copy in load_l[0]:
        copy.wait()
    for step in range(8):
        if step in (1, 2):
            load_mid[step].wait()
        if step == 3:
            for copy in load_l[1]:
                copy.wait()
        if step == 4:
            for side in range(2):
                halo[side].wait_recv()
                passed[side].start()
        if step == 5:
            load_low.wait()
            load_high.wait()
            for side in range(2):
                passed[side].wait_recv()
        compute(step)
        if step == 0:
            pl.when(late == 0)(enter)
        for copy in a_copies(step):
            copy.start()
        if step >= 1:
            reduce(step - 1)
    compute_own()
    own_copy().start()
    reduce(7)
    finish_own()
    for p in range(4):
        finish(p)
    for copy in halo + passed + [own_copy()]:
        copy.wait_send()
    for step in range(8):
        for copy in a_copies(step):
            copy.wait_send()
    for p in range(4):
        for copy in x_copies(p):
            copy.wait_send()
        for d in (1, 2, 3):
            y_copy(p, d).wait_send()


def shards(wavefunction, left_ops, right_ops, charge, couple, amplitude):
    ops, states = left_ops.shape[0], left_ops.shape[1]
    sectors = wavefunction.shape[0]
    stripe = states // lax.axis_size("op")
    left = left_ops.reshape(ops, 4, 2, 2 * stripe, states)
    smem = pl.BlockSpec(memory_space=pltpu.SMEM)
    hbm = pl.BlockSpec(memory_space=pl.ANY)
    dma = pltpu.SemaphoreType.DMA
    block = (states, states)
    return pl.pallas_call(
        kernel,
        out_shape=jax.ShapeDtypeStruct((sectors, stripe, states), F32),
        in_specs=[smem, smem, smem, hbm, hbm, hbm],
        out_specs=pl.BlockSpec(memory_space=pltpu.VMEM),
        scratch_shapes=[
            pltpu.VMEM((4, *block), BF16),
            pltpu.VMEM((4, *block), BF16),
            pltpu.VMEM((4, *block), BF16),
            pltpu.VMEM((3, *block), BF16),
            pltpu.VMEM((3, *block), BF16),
            pltpu.VMEM((2, 4, ops, 2 * stripe, states), BF16),
            pltpu.VMEM((states, ops * states), BF16),
            pltpu.VMEM((states, ops * states), BF16),
            pltpu.VMEM((states, ops * states), BF16),
            pltpu.VMEM((8, 2, 4, 2 * stripe, states), F32),
            pltpu.VMEM((8, 2 * stripe, states), F32),
            pltpu.VMEM((8, 2, 4, stripe, states), F32),
            pltpu.VMEM((8, stripe, states), F32),
            pltpu.VMEM((4, 4, 2 * stripe, states), BF16),
            pltpu.VMEM((4, 4, 2 * stripe, states), BF16),
            pltpu.VMEM((4, 3, 2 * stripe, states), BF16),
            pltpu.VMEM((4, 3, 2 * stripe, states), BF16),
            dma((5,)), dma((2, 4)), dma((ops,)), dma((2,)), dma((2,)), dma((2,)), dma((2,)), dma((8,)), dma((8,)),
            dma((3,)), dma((3,)), dma((2,)), dma((7,)), dma((7,)), dma((4, 3)), dma((4, 3)),
        ],
        compiler_params=pltpu.CompilerParams(
            collective_id=0, has_side_effects=True, vmem_limit_bytes=60000 * 1024
        ),
        name="sigma",
    )(charge, couple, amplitude, wavefunction, left, right_ops)


def solution(mesh):
    placed = (
        P("sec", None, None),
        P("op", None, None),
        P("op", None, None),
        P("op"),
        P("op", "sec"),
        P("op", "sec"),
    )
    return jax.shard_map(
        shards, mesh=mesh, in_specs=placed, out_specs=P("sec", "op", None), check_vma=False
    )
```

```python
import functools

import jax
import jax.numpy as jnp
from jax import lax
from jax.experimental import pallas as pl
from jax.experimental.pallas import tpu as pltpu
from jax.sharding import PartitionSpec as P

MESH = pl.DeviceIdType.MESH
F32 = jnp.float32
BF16 = jnp.bfloat16

PAIRS = ((1, 2), (3, 4), (5, 6), (0, 7))
STEPS = ((0, 0), (0, 1), (0, 2), (1, 0), (1, 1), (0, 3), (1, 2), (1, 3))
ORDER = (2, 1, 3)


def kernel(
    charge, couple, amplitude, wave, left, right, out,
    w_a, w_b, w_c, w_low, w_high, l_buf, r_buf, middle, own_middle, part, own_part, a_recv, own_recv,
    x_send, x_recv, y_send, y_recv,
    load_sem, l_sem, r_sem, halo_send, halo_recv, pass_send, pass_recv, a_ssem, a_rsem, last_ssem, last_rsem,
    own_sem, x_ssem, x_rsem, y_ssem, y_rsem,
):
    ops, states = right.shape[0], right.shape[1]
    stripe = out.shape[1]
    secs = lax.axis_size("sec")
    sec = lax.axis_index("sec")
    op = lax.axis_index("op")
    core = op % 2
    x = (op // 2) % 2
    y = op // 4
    core_peer = op + 1 - 2 * core
    x_peer = op + 2 - 4 * x
    depth = secs // 2
    to_right = {"sec": (sec + 1) % secs, "op": op + ((sec % depth) // (depth - 1)) * (x_peer - op)}
    to_left = {"sec": (sec + secs - 1) % secs, "op": op + ((depth - 1 - sec % depth) // (depth - 1)) * (x_peer - op)}
    y_peers = [((y + d) % 4) * 4 + x * 2 + core for d in (1, 2, 3)]

    barrier = pltpu.get_barrier_semaphore()
    for peer in (
        {"op": core_peer}, {"op": x_peer}, {"op": y_peers[0]}, {"op": y_peers[1]}, {"op": y_peers[2]},
        to_right, to_left,
    ):
        pl.semaphore_signal(barrier, inc=1, device_id=peer, device_id_type=MESH)

    sides = (1 - x, x)
    load_mid = [
        pltpu.make_async_copy(wave.at[pl.ds(2 * p, 4)], (w_a, w_b, w_c)[p], load_sem.at[p]) for p in range(3)
    ]
    load_low = pltpu.make_async_copy(wave.at[pl.ds(0, 2)], w_low.at[pl.ds(1, 2)], load_sem.at[3])
    load_high = pltpu.make_async_copy(wave.at[pl.ds(6, 2)], w_high.at[pl.ds(0, 2)], load_sem.at[4])
    load_l = [
        [
            pltpu.make_async_copy(left.at[:, (y + d) % 4, sides[half]], l_buf.at[half, d], l_sem.at[half, d])
            for d in range(4)
        ]
        for half in range(2)
    ]
    load_r = [
        pltpu.make_async_copy(right.at[k], r_buf.at[:, pl.ds(k * states, states)], r_sem.at[k])
        for k in range(ops)
    ]
    load_mid[0].start()
    for copy in load_l[0] + load_r:
        copy.start()
    for copy in (load_mid[1], load_mid[2], *load_l[1], load_low, load_high):
        copy.start()

    half_rows = pl.ds(pl.multiple_of(core * (states // 2), 8), states // 2)
    ends = (w_low.at[0, half_rows], w_high.at[2, half_rows])
    halo = [
        pltpu.make_async_remote_copy(
            wave.at[(7, 0)[side], half_rows], ends[side], halo_send.at[side], halo_recv.at[side],
            device_id=(to_right, to_left)[side], device_id_type=MESH,
        )
        for side in range(2)
    ]
    passed = [
        pltpu.make_async_remote_copy(
            ends[side], ends[side], pass_send.at[side], pass_recv.at[side],
            device_id={"op": core_peer}, device_id_type=MESH,
        )
        for side in range(2)
    ]

    def enter():
        pl.semaphore_wait(barrier, 7)
        for copy in halo:
            copy.start()

    late = (sec % depth) // (depth // 2)
    rows = 8 * stripe
    near = 2 * stripe

    def compute(step):
        half, p = STEPS[step]
        low, high, gap = ((w_a, w_a, 1), (w_b, w_b, 1), (w_c, w_c, 1), (w_low, w_high, 0))[p]
        skip = near * half
        kept = rows - skip
        for k in range(ops):
            at = 1 - charge[k]
            columns = slice(k * states, (k + 1) * states)
            blocks = jnp.concatenate([low[at], high[at + gap]], axis=1)
            product = jnp.dot(l_buf[half, :, k].reshape(rows, states), blocks, preferred_element_type=F32)
            product = product.astype(BF16).astype(F32)
            for j in range(2):
                target = PAIRS[p][j]
                factor = amplitude[k, target] * couple[k, target].astype(F32)
                scaled = (product[:, j * states : (j + 1) * states] * factor).astype(BF16)
                middle[j * kept : (j + 1) * kept, columns] = scaled[skip:]
                if half == 1:
                    own_middle[(2 * p + j) * near : (2 * p + j + 1) * near, columns] = scaled[:near]
        total = lax.dot_general(
            middle[: 2 * kept], r_buf[...], (((1,), (1,)), ((), ())), preferred_element_type=F32
        )
        part[step, :, half:] = total.reshape(2, 4 - half, near, states)

    def compute_own():
        total = lax.dot_general(
            own_middle[...], r_buf[...], (((1,), (1,)), ((), ())), preferred_element_type=F32
        )
        own_part[...] = total.reshape(own_part.shape)

    other = pl.ds(pl.multiple_of((1 - core) * stripe, 8), stripe)
    mine = pl.ds(pl.multiple_of(core * stripe, 8), stripe)

    def a_copies(step):
        if step == 7:
            return [
                pltpu.make_async_remote_copy(
                    part.at[step, :, d, other, :], a_recv.at[step, :, d], last_ssem.at[d - 1], last_rsem.at[d - 1],
                    device_id={"op": core_peer}, device_id_type=MESH,
                )
                for d in ORDER
            ]
        half = STEPS[step][0]
        return [
            pltpu.make_async_remote_copy(
                part.at[step, :, pl.ds(half, 4 - half), other, :], a_recv.at[step, :, pl.ds(half, 4 - half)],
                a_ssem.at[step], a_rsem.at[step],
                device_id={"op": core_peer}, device_id_type=MESH,
            )
        ]

    def own_copy():
        return pltpu.make_async_remote_copy(
            own_part.at[:, other, :], own_recv, own_sem.at[0], own_sem.at[1],
            device_id={"op": core_peer}, device_id_type=MESH,
        )

    def x_copies(p):
        if p == 3:
            return [
                pltpu.make_async_remote_copy(
                    x_send.at[p, d], x_recv.at[p, d], x_ssem.at[3 + d], x_rsem.at[3 + d],
                    device_id={"op": x_peer}, device_id_type=MESH,
                )
                for d in (*ORDER, 0)
            ]
        return [
            pltpu.make_async_remote_copy(
                x_send.at[p], x_recv.at[p], x_ssem.at[p], x_rsem.at[p],
                device_id={"op": x_peer}, device_id_type=MESH,
            )
        ]

    def y_copy(p, d):
        return pltpu.make_async_remote_copy(
            y_send.at[p, d - 1], y_recv.at[p, d - 1], y_ssem.at[p, d - 1], y_rsem.at[p, d - 1],
            device_id={"op": y_peers[d - 1]}, device_id_type=MESH,
        )

    def reduce(step):
        half, p = STEPS[step]
        core_copies = a_copies(step)
        across = x_copies(p)
        if step != 7:
            core_copies[0].wait_recv()
        if half == 1 and p != 3:
            across[0].wait_recv()
        for i, d in enumerate((*ORDER, 0) if half == 0 else ORDER):
            if step == 7:
                core_copies[i].wait_recv()
            value = jnp.concatenate([part[step, j, d, mine, :] + a_recv[step, j, d] for j in range(2)], axis=0)
            if half == 0:
                x_send[p, d] = value.astype(BF16)
                if p == 3:
                    across[i].start()
            else:
                if p == 3:
                    across[i].wait_recv()
                y_send[p, d - 1] = (value + x_recv[p, d].astype(F32)).astype(BF16)
                y_copy(p, d).start()
        if half == 0 and p != 3:
            across[0].start()

    def finish_own():
        own_copy().wait_recv()
        x_copies(3)[3].wait_recv()
        for p in range(4):
            for j in range(2):
                out[PAIRS[p][j]] = (
                    own_part[2 * p + j, mine, :]
                    + own_recv[2 * p + j]
                    + x_recv[p, 0, j * stripe : (j + 1) * stripe].astype(F32)
                )

    def finish(p):
        for d in (1, 3, 2):
            y_copy(p, d).wait_recv()
        value = y_recv[p, 0].astype(F32) + y_recv[p, 1].astype(F32) + y_recv[p, 2].astype(F32)
        for j in range(2):
            out[PAIRS[p][j]] += value[j * stripe : (j + 1) * stripe]

    pl.when(late == 1)(enter)
    load_mid[0].wait()
    for copy in load_l[0] + load_r:
        copy.wait()
    for step in range(8):
        if step in (1, 2):
            load_mid[step].wait()
        if step == 3:
            for copy in load_l[1]:
                copy.wait()
        if step == 4:
            for side in range(2):
                halo[side].wait_recv()
                passed[side].start()
        if step == 5:
            load_low.wait()
            load_high.wait()
            for side in range(2):
                passed[side].wait_recv()
        compute(step)
        if step == 0:
            pl.when(late == 0)(enter)
        for copy in a_copies(step):
            copy.start()
        if step >= 1:
            reduce(step - 1)
    compute_own()
    own_copy().start()
    reduce(7)
    finish_own()
    for p in range(4):
        finish(p)
    for copy in halo + passed + [own_copy()]:
        copy.wait_send()
    for step in range(8):
        for copy in a_copies(step):
            copy.wait_send()
    for p in range(4):
        for copy in x_copies(p):
            copy.wait_send()
        for d in (1, 2, 3):
            y_copy(p, d).wait_send()


def shards(wavefunction, left_ops, right_ops, charge, couple, amplitude):
    ops, states = left_ops.shape[0], left_ops.shape[1]
    sectors = wavefunction.shape[0]
    stripe = states // lax.axis_size("op")
    left = left_ops.reshape(ops, 4, 2, 2 * stripe, states)
    smem = pl.BlockSpec(memory_space=pltpu.SMEM)
    hbm = pl.BlockSpec(memory_space=pl.ANY)
    dma = pltpu.SemaphoreType.DMA
    block = (states, states)
    return pl.pallas_call(
        kernel,
        out_shape=jax.ShapeDtypeStruct((sectors, stripe, states), F32),
        in_specs=[smem, smem, smem, hbm, hbm, hbm],
        out_specs=pl.BlockSpec(memory_space=pltpu.VMEM),
        scratch_shapes=[
            pltpu.VMEM((4, *block), BF16),
            pltpu.VMEM((4, *block), BF16),
            pltpu.VMEM((4, *block), BF16),
            pltpu.VMEM((3, *block), BF16),
            pltpu.VMEM((3, *block), BF16),
            pltpu.VMEM((2, 4, ops, 2 * stripe, states), BF16),
            pltpu.VMEM((states, ops * states), BF16),
            pltpu.VMEM((states, ops * states), BF16),
            pltpu.VMEM((states, ops * states), BF16),
            pltpu.VMEM((8, 2, 4, 2 * stripe, states), F32),
            pltpu.VMEM((8, 2 * stripe, states), F32),
            pltpu.VMEM((8, 2, 4, stripe, states), F32),
            pltpu.VMEM((8, stripe, states), F32),
            pltpu.VMEM((4, 4, 2 * stripe, states), BF16),
            pltpu.VMEM((4, 4, 2 * stripe, states), BF16),
            pltpu.VMEM((4, 3, 2 * stripe, states), BF16),
            pltpu.VMEM((4, 3, 2 * stripe, states), BF16),
            dma((5,)), dma((2, 4)), dma((ops,)), dma((2,)), dma((2,)), dma((2,)), dma((2,)), dma((8,)), dma((8,)),
            dma((3,)), dma((3,)), dma((2,)), dma((7,)), dma((7,)), dma((4, 3)), dma((4, 3)),
        ],
        compiler_params=pltpu.CompilerParams(
            collective_id=0, has_side_effects=True, vmem_limit_bytes=60000 * 1024
        ),
        name="sigma",
    )(charge, couple, amplitude, wavefunction, left, right_ops)


def solution(mesh):
    placed = (
        P("sec", None, None),
        P("op", None, None),
        P("op", None, None),
        P("op"),
        P("op", "sec"),
        P("op", "sec"),
    )
    return jax.shard_map(
        shards, mesh=mesh, in_specs=placed, out_specs=P("sec", "op", None), check_vma=False
    )
```
